512 devices in a mesh: groups: 2 (over y), seq: 16 (over z), head: 8 (over x), layer: 2 (over core).
Axes of the slice: x: 8, y: 2, z: 16, core: 2. Of those that a mesh axis runs over, the one named last changes fastest.
The devices are a block of a 8x16x16 slice.
Arguments:
- kv_cache: bfloat16 [2, 2, 8, 16384, 8, 128], P(None, 'layer', 'groups', 'seq', 'head'), parts along dimension 2, may hold values from -800 to 800
- valid_blocks: int32 [8], P('groups'), parts along dimension 0, may hold values from 1 to 128, 256 in all
Outputs:
- decode_cache: bfloat16 [2, 2, 32, 4096, 8, 128], P(None, 'layer', ('groups', 'seq'), None, 'head'), parts along dimension 2
- centers: float32 [2, 2, 8, 8, 128], P(None, 'layer', 'groups', 'head'), parts along dimension 2
- scales: float32 [2, 2, 8, 8, 128], P(None, 'layer', 'groups', 'head'), parts along dimension 2
The draws below stay inside these ranges and needn't reach their ends.
There are 2 independent parts, one for each index of `groups`. The reference program is written for one: setup_inputs(seed, part) draws one part's arguments, and reference() takes and returns one part's arrays. A program takes and returns all parts, laid end to end along the dimension named above; each array names one. Nothing has to cross between parts.
Inputs may be any that keep to these rules, and one draw needn't show every extreme that they name: `valid_blocks`: the counts of the 4 users sum to 256, and the largest equals 128.
All inputs are finite; a program needn't handle non-finite values.
Results may differ from the reference program's by a relative error of at most 0.001.
Values may be sent and summed in bfloat16 or wider, within the bound.
A program may use at most 64 MiB of HBM per device.

```python
import math
import jax
import jax.numpy as jnp
import numpy as np

HEAD = 128
KVH = 8
LAYERS = 2
USERS = 4
PDEV = 1024
BLOCK = 128
SEQ = 16384
NBLK = 128
N_SEQ = 16


def draw_kv_cache(key, part):
    shape = (2, LAYERS, USERS, SEQ, KVH, HEAD)
    row_shape = (2, LAYERS, USERS, SEQ, KVH, 1)
    col_shape = (2, LAYERS, USERS, 1, KVH, HEAD)
    keys = jax.random.split(jax.random.fold_in(key, 11), 4)
    cols = jnp.exp(jax.random.uniform(keys[1], col_shape, jnp.float32, 0.0, math.log(10.0)))
    trend = 1.0 + 2.0 * jnp.arange(SEQ, dtype=jnp.float32).reshape(1, 1, 1, SEQ, 1, 1) / SEQ
    rows = jnp.exp(jax.random.uniform(keys[0], row_shape, jnp.float32, 0.0, math.log(10.0)))
    noise = jnp.clip(jax.random.normal(keys[2], shape, jnp.float32), -4.0, 4.0)
    offset = jnp.clip(jax.random.normal(keys[3], col_shape, jnp.float32), -4.0, 4.0) * 3.0 * cols
    value = trend * (offset + 0.3 * rows * cols * noise)
    return value.astype(jnp.bfloat16)


def split_up(amount, total, reach, skew):
    portions = [(1 << 20) // math.isqrt(standing ** skew) + 1 for standing in range(2, amount + 1)]
    spare, counts = total - reach - (amount - 1), [1] * (amount - 1)
    while spare > 0:
        candidates = [i for i in range(amount - 1) if counts[i] < reach]
        pool, remaining = sum([portions[i] for i in candidates]), spare
        for i in candidates:
            more = min(reach - counts[i], max(1, remaining * portions[i] // pool), spare)
            counts[i] = counts[i] + more
            spare = spare - more
    return np.array([reach] + counts)


def uneven_parts(key, count, total, limit, lean):
    if count == 2:
        one = jax.random.randint(key, (), max(1, total - limit), min(limit, total - 1) + 1)
        return jnp.stack([one, total - one])
    sizes = jnp.asarray(split_up(count, total, limit, lean), jnp.int32)
    pairs = (count - 1) // 2
    donor, sink = sizes[1:1 + 2 * pairs:2], sizes[2:2 + 2 * pairs:2]
    margin = jnp.minimum(donor - 1, limit - sink)
    shifted = jax.random.randint(jax.random.fold_in(key, 1), (pairs,), 0, 1 << 20) % (margin + 1)
    sizes = sizes.at[1:1 + 2 * pairs:2].set(donor - shifted).at[2:2 + 2 * pairs:2].set(sink + shifted)
    return sizes[jax.random.permutation(jax.random.fold_in(key, 2), count)]


def setup_inputs(seed: int = 0, part: int = 0) -> dict:
    key_list = jax.random.split(jax.random.key(seed), 3)
    part_keys = jax.random.split(jax.random.fold_in(key_list[2], part), 3)
    return {
        "kv_cache": draw_kv_cache(jax.random.fold_in(jax.random.fold_in(key_list[2], part), 71), part),
        "valid_blocks": uneven_parts(part_keys[1], USERS, USERS * NBLK // 2, NBLK, 2).astype(jnp.int32),
    }


epsilon = 1e-6


def reference(kv_cache, valid_blocks):
    lengths = valid_blocks.astype(jnp.int32) * BLOCK
    values = kv_cache.astype(jnp.float32)
    position = jnp.arange(SEQ, dtype=jnp.int32)
    is_live = position[None, :] < lengths[:, None]
    live_mask = is_live[None, None, :, :, None, None]
    totals = jnp.sum(jnp.where(live_mask, values, 0.0), axis=3)
    centers = totals / lengths.astype(jnp.float32)[None, None, :, None, None]
    spread = jnp.max(jnp.where(live_mask, jnp.abs(values - centers[:, :, :, None]), 0.0), axis=3)
    scales = spread + epsilon
    normed = jnp.where(live_mask, (values - centers[:, :, :, None]) / scales[:, :, :, None], 0.0).astype(jnp.bfloat16)
    owns = N_SEQ // USERS
    slice_len = PDEV // owns
    shaped = normed.reshape(2, LAYERS, USERS, N_SEQ, owns, slice_len, KVH, HEAD)
    shaped = jnp.transpose(shaped, (0, 1, 2, 4, 3, 5, 6, 7))
    decode_cache = shaped.reshape(2, LAYERS, USERS * owns, N_SEQ * slice_len, KVH, HEAD)
    return decode_cache, centers, scales
```

```python
import functools

import jax
import jax.numpy as jnp
from jax import lax
from jax.experimental import pallas as pl
from jax.experimental.pallas import tpu as pltpu
from jax.sharding import PartitionSpec as P

BLOCK = 128

epsilon = 1e-06
ceiling_value = 3e38
ROOT = 0


def exchange_kernel(
    n,
    kv_ref,
    blocks_ref,
    recv_ref,
    finals_ref,
    local,
    mine,
    gathered,
    finals,
    load_sem,
    own_sem,
    send_sem,
    recv_sem,
    stat_send_sem,
    stat_recv_sem,
    final_send_sem,
    final_recv_sem,
    ready,
):
    kinds, owners, part_len, head_dim = kv_ref.shape
    users = blocks_ref.shape[0]
    quarter = owners // users
    per_part = part_len // BLOCK
    per_dev = quarter * per_part
    rows = kinds * users
    z = lax.axis_index("seq")

    load = pltpu.make_async_copy(kv_ref, local, load_sem)
    load.start()

    barrier = pltpu.get_barrier_semaphore()

    @pl.when(z > 0)
    def _():
        pl.semaphore_wait(barrier, 1)

    @pl.when(z < n - 1)
    def _():
        pl.semaphore_signal(barrier, inc=1, device_id={"seq": z + 1})

    def announce(s, carry):
        pl.semaphore_signal(ready.at[z], inc=1, device_id={"seq": s})
        return carry

    lax.fori_loop(0, z, announce, 0)

    def bulk(t):
        return pltpu.make_async_remote_copy(
            src_ref=kv_ref.at[:, t],
            dst_ref=recv_ref.at[:, z],
            send_sem=send_sem.at[t],
            recv_sem=recv_sem.at[z],
            device_id={"seq": t},
        )

    @pl.when(z > 0)
    def _():
        bulk(0).start()

    load.wait()
    own = pltpu.make_async_copy(local.at[:, z], recv_ref.at[:, z], own_sem)
    own.start()

    def one_row(r, carry):
        k, u = r // users, r % users
        total = jnp.zeros((8, head_dim), jnp.float32)
        high = jnp.full((8, head_dim), -ceiling_value, jnp.float32)
        low = jnp.full((8, head_dim), ceiling_value, jnp.float32)
        count = blocks_ref[u]
        for b in range(per_dev):
            part = local[
                k,
                u * quarter + b // per_part,
                (b % per_part) * BLOCK : (b % per_part + 1) * BLOCK,
                :,
            ].astype(jnp.float32)
            part = part.reshape(BLOCK // 8, 8, head_dim)
            alive = z * per_dev + b < count
            total += jnp.where(alive, jnp.sum(part, axis=0), 0.0)
            high = jnp.maximum(high, jnp.where(alive, jnp.max(part, axis=0), -ceiling_value))
            low = jnp.minimum(low, jnp.where(alive, jnp.min(part, axis=0), ceiling_value))
        mine[0, pl.ds(r, 1), :] = jnp.sum(total, axis=0, keepdims=True)
        mine[1, pl.ds(r, 1), :] = jnp.max(high, axis=0, keepdims=True)
        mine[2, pl.ds(r, 1), :] = jnp.min(low, axis=0, keepdims=True)
        return carry

    lax.fori_loop(0, rows, one_row, 0)

    def stat_copy():
        return pltpu.make_async_remote_copy(
            src_ref=mine,
            dst_ref=gathered.at[z],
            send_sem=stat_send_sem,
            recv_sem=stat_recv_sem.at[z],
            device_id={"seq": ROOT},
        )

    @pl.when(z != ROOT)
    def _():
        stat_copy().start()

    def send_lower(t, carry):
        bulk(t).start()
        return carry

    lax.fori_loop(1, z, send_lower, 0)

    def send_upper(t, carry):
        pl.semaphore_wait(ready.at[t], 1)
        bulk(t).start()
        return carry

    lax.fori_loop(z + 1, n, send_upper, 0)

    def final_copy(t):
        return pltpu.make_async_remote_copy(
            src_ref=finals,
            dst_ref=finals,
            send_sem=final_send_sem.at[t],
            recv_sem=final_recv_sem,
            device_id={"seq": t},
        )

    @pl.when(z == ROOT)
    def _():
        def merge(s, carry):
            total, high, low = carry
            pltpu.make_async_remote_copy(
                src_ref=mine,
                dst_ref=gathered.at[s],
                send_sem=stat_send_sem,
                recv_sem=stat_recv_sem.at[s],
                device_id={"seq": ROOT},
            ).wait_recv()
            return (
                total + gathered[s, 0],
                jnp.maximum(high, gathered[s, 1]),
                jnp.minimum(low, gathered[s, 2]),
            )

        total, high, low = lax.fori_loop(1, n, merge, (mine[0], mine[1], mine[2]))
        row = lax.broadcasted_iota(jnp.int32, (rows, head_dim), 0)
        length = jnp.zeros((rows, head_dim), jnp.float32)
        for u in range(users):
            tokens = (blocks_ref[u] * BLOCK).astype(jnp.float32)
            length = jnp.where(row % users == u, tokens, length)
        center = total / length
        finals[0] = center
        finals[1] = jnp.maximum(high - center, center - low) + epsilon

        def send_final(t, carry):
            final_copy(t).start()
            return carry

        lax.fori_loop(1, n, send_final, 0)

        def drain_final(t, carry):
            final_copy(t).wait_send()
            return carry

        lax.fori_loop(1, n, drain_final, 0)

    @pl.when(z != ROOT)
    def _():
        final_copy(0).wait_recv()
        stat_copy().wait_send()

    finals_ref[...] = finals[...]

    def drain(t, carry):
        @pl.when(t != z)
        def _():
            bulk(t).wait_send()
            pltpu.make_async_remote_copy(
                src_ref=kv_ref.at[:, t],
                dst_ref=recv_ref.at[:, t],
                send_sem=send_sem.at[t],
                recv_sem=recv_sem.at[t],
                device_id={"seq": t},
            ).wait_recv()

        return carry

    lax.fori_loop(0, n, drain, 0)
    own.wait()


def on_device(kv_cache, valid_blocks):
    kinds, layer_dev, users, per_dev, heads_dev, head_dim = kv_cache.shape
    n = lax.axis_size("seq")
    quarter = n // users
    part_len = per_dev // quarter
    rows = kinds * users
    kv = kv_cache.reshape(kinds, n, part_len, head_dim)
    recv, finals = pl.pallas_call(
        functools.partial(exchange_kernel, n),
        out_shape=(
            jax.ShapeDtypeStruct((kinds, n, part_len, head_dim), kv.dtype),
            jax.ShapeDtypeStruct((2, rows, head_dim), jnp.float32),
        ),
        in_specs=[
            pl.BlockSpec(memory_space=pl.ANY),
            pl.BlockSpec(memory_space=pltpu.SMEM),
        ],
        out_specs=(
            pl.BlockSpec(memory_space=pl.ANY),
            pl.BlockSpec(memory_space=pltpu.VMEM),
        ),
        scratch_shapes=[
            pltpu.VMEM((kinds, n, part_len, head_dim), kv.dtype),
            pltpu.VMEM((3, rows, head_dim), jnp.float32),
            pltpu.VMEM((n, 3, rows, head_dim), jnp.float32),
            pltpu.VMEM((2, rows, head_dim), jnp.float32),
            pltpu.SemaphoreType.DMA,
            pltpu.SemaphoreType.DMA,
            pltpu.SemaphoreType.DMA((n,)),
            pltpu.SemaphoreType.DMA((n,)),
            pltpu.SemaphoreType.DMA,
            pltpu.SemaphoreType.DMA((n,)),
            pltpu.SemaphoreType.DMA((n,)),
            pltpu.SemaphoreType.DMA,
            pltpu.SemaphoreType.REGULAR((n,)),
        ],
        compiler_params=pltpu.CompilerParams(collective_id=0, has_side_effects=True),
    )(kv, valid_blocks)
    z = lax.axis_index("seq")
    user = z // quarter
    per_row = finals.reshape(2, kinds, users, head_dim)
    mine = lax.dynamic_slice_in_dim(per_row, user, 1, axis=2)[:, :, :, None, :]
    length = lax.dynamic_slice_in_dim(valid_blocks, user, 1)[0] * BLOCK
    source = jnp.arange(n, dtype=jnp.int32)[:, None]
    offset = jnp.arange(part_len, dtype=jnp.int32)[None, :]
    position = source * per_dev + (z % quarter) * part_len + offset
    live = (position < length)[None, :, :, None]
    normed = jnp.where(live, (recv.astype(jnp.float32) - mine[0]) / mine[1], 0.0)
    arranged = normed.astype(kv_cache.dtype).reshape(
        kinds, layer_dev, 1, n * part_len, heads_dev, head_dim
    )
    outs = finals.reshape(2, kinds, layer_dev, users, heads_dev, head_dim)
    return (arranged, outs[0], outs[1])


def solution(mesh):
    in_specs = (P(None, "layer", "groups", "seq", "head", None), P("groups"))
    out_specs = (
        P(None, "layer", ("groups", "seq"), None, "head", None),
        P(None, "layer", "groups", "head", None),
        P(None, "layer", "groups", "head", None),
    )
    return jax.shard_map(
        on_device, mesh=mesh, in_specs=in_specs, out_specs=out_specs, check_vma=False
    )
```

```python
import functools

import jax
import jax.numpy as jnp
from jax import lax
from jax.experimental import pallas as pl
from jax.experimental.pallas import tpu as pltpu
from jax.sharding import PartitionSpec as P

BLOCK = 128

epsilon = 1e-06
ceiling_value = 3e38
KEEP = 2


def exchange_kernel(
    n,
    kv_ref,
    blocks_ref,
    out_ref,
    centers_ref,
    scales_ref,
    local,
    recv,
    done,
    mine,
    gathered,
    finals,
    load_sem,
    own_sem,
    out_sem,
    send_sem,
    recv_sem,
    stat_send_sem,
    stat_recv_sem,
    final_send_sem,
    final_recv_sem,
    ready,
    token,
):
    kinds, owners, part_len, head_dim = kv_ref.shape
    users = blocks_ref.shape[0]
    quarter = owners // users
    per_part = part_len // BLOCK
    per_dev = quarter * per_part
    rows = kinds * users
    half = n // 2
    z = lax.axis_index("seq")
    my_user, my_part = z // quarter, z % quarter
    early = z < half

    load = pltpu.make_async_copy(kv_ref, local, load_sem)
    load.start()
    own = pltpu.make_async_copy(kv_ref.at[:, z], recv.at[:, z], own_sem)
    own.start()

    barrier = pltpu.get_barrier_semaphore()

    @pl.when(z > 0)
    def _():
        pl.semaphore_wait(barrier, 1)

    @pl.when(z < n - 1)
    def _():
        pl.semaphore_signal(barrier, inc=1, device_id={"seq": z + 1})

    def announce(s, carry):
        pl.semaphore_signal(ready.at[z], inc=1, device_id={"seq": s})
        return carry

    lax.fori_loop(0, z, announce, 0)

    def bulk(t, k, s=None):
        s = z if s is None else s
        return pltpu.make_async_remote_copy(
            src_ref=kv_ref.at[k, t],
            dst_ref=recv.at[k, s],
            send_sem=send_sem.at[k, t],
            recv_sem=recv_sem.at[k, s],
            device_id={"seq": t},
        )

    def send_part(t, carry):
        for k in range(kinds):
            bulk(t, k).start()
        return carry

    late = jnp.logical_and(z > half, z < n - 1)

    @pl.when(late)
    def _():
        send_part(0, 0)

    near = jnp.maximum(z - half + 1 - z % 2, 0)

    @pl.when(z < n - 1)
    def _():
        lax.fori_loop(near, z, send_part, 0)

    load.wait()

    def one_row(r, carry):
        k, u = r // users, r % users
        total = jnp.zeros((8, head_dim), jnp.float32)
        high = jnp.full((8, head_dim), -ceiling_value, jnp.float32)
        low = jnp.full((8, head_dim), ceiling_value, jnp.float32)
        count = blocks_ref[u]
        for b in range(per_dev):
            part = local[
                k,
                u * quarter + b // per_part,
                (b % per_part) * BLOCK : (b % per_part + 1) * BLOCK,
                :,
            ].astype(jnp.float32)
            part = part.reshape(BLOCK // 8, 8, head_dim)
            alive = z * per_dev + b < count
            total += jnp.where(alive, jnp.sum(part, axis=0), 0.0)
            high = jnp.maximum(high, jnp.where(alive, jnp.max(part, axis=0), -ceiling_value))
            low = jnp.minimum(low, jnp.where(alive, jnp.min(part, axis=0), ceiling_value))
        mine[0, pl.ds(r, 1), :] = jnp.sum(total, axis=0, keepdims=True)
        mine[1, pl.ds(r, 1), :] = jnp.max(high, axis=0, keepdims=True)
        mine[2, pl.ds(r, 1), :] = jnp.min(low, axis=0, keepdims=True)
        return carry

    lax.fori_loop(0, rows, one_row, 0)

    def prefix(s):
        return pltpu.make_async_remote_copy(
            src_ref=mine,
            dst_ref=gathered,
            send_sem=stat_send_sem,
            recv_sem=stat_recv_sem,
            device_id={"seq": s + 1},
        )

    @pl.when(z > 0)
    def _():
        prefix(z - 1).wait_recv()
        mine[0] = mine[0] + gathered[0]
        mine[1] = jnp.maximum(mine[1], gathered[1])
        mine[2] = jnp.minimum(mine[2], gathered[2])

    def final(t):
        return pltpu.make_async_remote_copy(
            src_ref=finals,
            dst_ref=finals,
            send_sem=final_send_sem.at[t],
            recv_sem=final_recv_sem,
            device_id={"seq": t},
        )

    @pl.when(z < n - 1)
    def _():
        pl.semaphore_wait(ready.at[z + 1], 1)
        prefix(z).start()

    @pl.when(z == n - 1)
    def _():
        row = lax.broadcasted_iota(jnp.int32, (rows, head_dim), 0)
        length = jnp.zeros((rows, head_dim), jnp.float32)
        for u in range(users):
            tokens = (blocks_ref[u] * BLOCK).astype(jnp.float32)
            length = jnp.where(row % users == u, tokens, length)
        center = mine[0] / length
        finals[0] = center
        finals[1] = jnp.maximum(mine[1] - center, center - mine[2]) + epsilon

        def send_final(t, carry):
            final(t).start()
            return carry

        lax.fori_loop(0, n - 1, send_final, 0)

    lax.fori_loop(jnp.where(late, 1, 0), near, send_part, 0)

    @pl.when(z == n - 1)
    def _():
        lax.fori_loop(near, z, send_part, 0)

    far = z + half + 1 - z % 2

    def send_upper(t, carry):
        @pl.when(t > z + 1)
        def _():
            pl.semaphore_wait(ready.at[t], 1)

        @pl.when(jnp.logical_or(z == 0, jnp.logical_or(z >= half, t < far)))
        def _():
            send_part(t, 0)

        return carry

    lax.fori_loop(z + 1, n, send_upper, 0)

    def in_turn():
        @pl.when(z > 0)
        def _():
            pl.semaphore_wait(token, 1)
            lax.fori_loop(far, n, send_part, 0)

        @pl.when(z < half - 1)
        def _():
            def drain_far(i, carry):
                bulk(i // kinds, i % kinds).wait_send()
                return carry

            lax.fori_loop(far * kinds, n * kinds - KEEP, drain_far, 0)
            pl.semaphore_signal(token, inc=1, device_id={"seq": z + 1})

    @pl.when(z < half // 2)
    def _():
        in_turn()

    @pl.when(z < n - 1)
    def _():
        final(z).wait_recv()

    my_count = blocks_ref[my_user]
    centers = [finals[0, pl.ds(k * users + my_user, 1), :] for k in range(kinds)]
    scales = [finals[1, pl.ds(k * users + my_user, 1), :] for k in range(kinds)]

    def normalise(s, carry):
        @pl.when(s == z)
        def _():
            own.wait()

        @pl.when(s != z)
        def _():
            for k in range(kinds):
                bulk(s, k, s).wait_recv()

        for k in range(kinds):
            for b in range(per_part):
                span = slice(b * BLOCK, (b + 1) * BLOCK)
                value = recv[k, s, span, :].astype(jnp.float32)
                scaled = (value - centers[k]) / scales[k]
                alive = s * per_dev + my_part * per_part + b < my_count
                done[k, s, span, :] = jnp.where(alive, scaled, 0.0).astype(done.dtype)
        pltpu.make_async_copy(done.at[:, s], out_ref.at[:, s], out_sem.at[s]).start()
        return carry

    lax.fori_loop(0, z + 1, normalise, 0)

    @pl.when(jnp.logical_and(z >= half // 2, early))
    def _():
        in_turn()

    for k in range(kinds):
        centers_ref[k] = finals[0, k * users : (k + 1) * users, :]
        scales_ref[k] = finals[1, k * users : (k + 1) * users, :]

    lax.fori_loop(z + 1, n, normalise, 0)

    @pl.when(z < n - 1)
    def _():
        prefix(z).wait_send()

    @pl.when(z == n - 1)
    def _():
        def drain_final(t, carry):
            final(t).wait_send()
            return carry

        lax.fori_loop(0, n - 1, drain_final, 0)

    def drain(t, carry):
        for k in range(kinds):
            waited = jnp.logical_and(
                jnp.logical_and(z < half - 1, t >= far), t * kinds + k < n * kinds - KEEP
            )

            @pl.when(jnp.logical_not(jnp.logical_or(waited, t == z)))
            def _(k=k):
                bulk(t, k).wait_send()

        pltpu.make_async_copy(done.at[:, t], out_ref.at[:, t], out_sem.at[t]).wait()
        return carry

    lax.fori_loop(0, n, drain, 0)


def on_device(kv_cache, valid_blocks):
    kinds, layer_dev, users, per_dev, heads_dev, head_dim = kv_cache.shape
    n = lax.axis_size("seq")
    part_len = per_dev // (n // users)
    kv = kv_cache.reshape(kinds, n, part_len, head_dim)
    whole = (kinds, n, part_len, head_dim)
    rows = kinds * users
    dma = pltpu.SemaphoreType.DMA
    out, centers, scales = pl.pallas_call(
        functools.partial(exchange_kernel, n),
        out_shape=(
            jax.ShapeDtypeStruct(whole, kv.dtype),
            jax.ShapeDtypeStruct((kinds, users, head_dim), jnp.float32),
            jax.ShapeDtypeStruct((kinds, users, head_dim), jnp.float32),
        ),
        in_specs=[
            pl.BlockSpec(memory_space=pl.ANY),
            pl.BlockSpec(memory_space=pltpu.SMEM),
        ],
        out_specs=(
            pl.BlockSpec(memory_space=pl.ANY),
            pl.BlockSpec(memory_space=pltpu.VMEM),
            pl.BlockSpec(memory_space=pltpu.VMEM),
        ),
        scratch_shapes=[
            pltpu.VMEM(whole, kv.dtype),
            pltpu.VMEM(whole, kv.dtype),
            pltpu.VMEM(whole, kv.dtype),
            pltpu.VMEM((3, rows, head_dim), jnp.float32),
            pltpu.VMEM((3, rows, head_dim), jnp.float32),
            pltpu.VMEM((2, rows, head_dim), jnp.float32),
            dma,
            dma,
            dma((n,)),
            dma((kinds, n)),
            dma((kinds, n)),
            dma,
            dma,
            dma((n,)),
            dma,
            pltpu.SemaphoreType.REGULAR((n,)),
            pltpu.SemaphoreType.REGULAR,
        ],
        compiler_params=pltpu.CompilerParams(collective_id=0, has_side_effects=True),
    )(kv, valid_blocks)
    arranged = out.reshape(kinds, layer_dev, 1, n * part_len, heads_dev, head_dim)
    small = (kinds, layer_dev, users, heads_dev, head_dim)
    return (arranged, centers.reshape(small), scales.reshape(small))


def solution(mesh):
    in_specs = (P(None, "layer", "groups", "seq", "head", None), P("groups"))
    out_specs = (
        P(None, "layer", ("groups", "seq"), None, "head", None),
        P(None, "layer", "groups", "head", None),
        P(None, "layer", "groups", "head", None),
    )
    return jax.shard_map(
        on_device, mesh=mesh, in_specs=in_specs, out_specs=out_specs, check_vma=False
    )
```

```python
import functools

import jax
import jax.numpy as jnp
from jax import lax
from jax.experimental import pallas as pl
from jax.experimental.pallas import tpu as pltpu
from jax.sharding import PartitionSpec as P

BLOCK = 128

epsilon = 1e-06
ceiling_value = 3e38
KEEP = (1, 2)
VMEM_LIMIT = 51 * 1024 * 1024


def exchange_kernel(
    n,
    kv_ref,
    blocks_ref,
    out_ref,
    finals_ref,
    local,
    recv,
    mine,
    gathered,
    finals,
    load_sem,
    own_sem,
    send_sem,
    recv_sem,
    stat_send_sem,
    stat_recv_sem,
    final_send_sem,
    final_recv_sem,
    ready,
    token,
):
    kinds, owners, part_len, head_dim = kv_ref.shape
    users = blocks_ref.shape[0]
    quarter = owners // users
    per_part = part_len // BLOCK
    per_dev = quarter * per_part
    rows = kinds * users
    half = n // 2
    z = lax.axis_index("seq")
    my_user, my_part = z // quarter, z % quarter
    early = z < half
    keep = jnp.where(z == 0, KEEP[0], KEEP[1])

    load = pltpu.make_async_copy(kv_ref, local, load_sem)
    load.start()
    own = pltpu.make_async_copy(kv_ref.at[:, z], recv.at[:, z], own_sem)
    own.start()

    barrier = pltpu.get_barrier_semaphore()

    @pl.when(z > 0)
    def _():
        pl.semaphore_wait(barrier, 1)

    @pl.when(z < n - 1)
    def _():
        pl.semaphore_signal(barrier, inc=1, device_id={"seq": z + 1})

    def announce(s, carry):
        pl.semaphore_signal(ready.at[z], inc=1, device_id={"seq": s})
        return carry

    lax.fori_loop(0, z, announce, 0)

    def bulk(t, k, s=None):
        s = z if s is None else s
        return pltpu.make_async_remote_copy(
            src_ref=kv_ref.at[k, t],
            dst_ref=recv.at[k, s],
            send_sem=send_sem.at[k, t],
            recv_sem=recv_sem.at[k, s],
            device_id={"seq": t},
        )

    def send_part(t, carry):
        for k in range(kinds):
            bulk(t, k).start()
        return carry

    late = jnp.logical_and(z >= half, z < n - 1)

    @pl.when(late)
    def _():
        send_part(0, 0)

    near = jnp.maximum(z - half + 1 - z % 2, 0)

    @pl.when(z < n - 1)
    def _():
        lax.fori_loop(near, z, send_part, 0)

    load.wait()

    def one_row(r, carry):
        k, u = r // users, r % users
        total = jnp.zeros((8, head_dim), jnp.float32)
        high = jnp.full((8, head_dim), -ceiling_value, jnp.float32)
        low = jnp.full((8, head_dim), ceiling_value, jnp.float32)
        count = blocks_ref[u]
        for b in range(per_dev):
            part = local[
                k,
                u * quarter + b // per_part,
                (b % per_part) * BLOCK : (b % per_part + 1) * BLOCK,
                :,
            ].astype(jnp.float32)
            part = part.reshape(BLOCK // 8, 8, head_dim)
            alive = z * per_dev + b < count
            total += jnp.where(alive, jnp.sum(part, axis=0), 0.0)
            high = jnp.maximum(high, jnp.where(alive, jnp.max(part, axis=0), -ceiling_value))
            low = jnp.minimum(low, jnp.where(alive, jnp.min(part, axis=0), ceiling_value))
        mine[0, pl.ds(r, 1), :] = jnp.sum(total, axis=0, keepdims=True)
        mine[1, pl.ds(r, 1), :] = jnp.max(high, axis=0, keepdims=True)
        mine[2, pl.ds(r, 1), :] = jnp.min(low, axis=0, keepdims=True)
        return carry

    lax.fori_loop(0, rows, one_row, 0)

    def prefix(s):
        return pltpu.make_async_remote_copy(
            src_ref=mine,
            dst_ref=gathered,
            send_sem=stat_send_sem,
            recv_sem=stat_recv_sem,
            device_id={"seq": s + 1},
        )

    @pl.when(z > 0)
    def _():
        prefix(z - 1).wait_recv()
        mine[0] = mine[0] + gathered[0]
        mine[1] = jnp.maximum(mine[1], gathered[1])
        mine[2] = jnp.minimum(mine[2], gathered[2])

    def final(t):
        return pltpu.make_async_remote_copy(
            src_ref=finals,
            dst_ref=finals,
            send_sem=final_send_sem.at[t],
            recv_sem=final_recv_sem,
            device_id={"seq": t},
        )

    @pl.when(z < n - 1)
    def _():
        pl.semaphore_wait(ready.at[z + 1], 1)
        prefix(z).start()

    @pl.when(z == n - 1)
    def _():
        row = lax.broadcasted_iota(jnp.int32, (rows, head_dim), 0)
        length = jnp.zeros((rows, head_dim), jnp.float32)
        for u in range(users):
            tokens = (blocks_ref[u] * BLOCK).astype(jnp.float32)
            length = jnp.where(row % users == u, tokens, length)
        center = mine[0] / length
        finals[0] = center
        finals[1] = jnp.maximum(mine[1] - center, center - mine[2]) + epsilon

        def send_final(t, carry):
            final(t).start()
            return carry

        lax.fori_loop(0, n - 1, send_final, 0)

    lax.fori_loop(jnp.where(late, 1, 0), near, send_part, 0)

    @pl.when(z == n - 1)
    def _():
        lax.fori_loop(near, z, send_part, 0)

    far = z + half + 1 - z % 2

    def send_upper(t, carry):
        @pl.when(t > z + 1)
        def _():
            pl.semaphore_wait(ready.at[t], 1)

        @pl.when(jnp.logical_and(early, jnp.logical_or(t <= half, jnp.logical_and(z == 0, t >= far))))
        def _():
            send_part(t, 0)

        return carry

    lax.fori_loop(z + 1, n, send_upper, 0)
    lax.fori_loop(jnp.maximum(z, half) + 1, jnp.minimum(far, n), send_part, 0)

    def in_turn():
        @pl.when(z > 0)
        def _():
            pl.semaphore_wait(token, 1)
            lax.fori_loop(far, n, send_part, 0)

        @pl.when(z < half - 1)
        def _():
            def drain_far(i, carry):
                bulk(i // kinds, i % kinds).wait_send()
                return carry

            lax.fori_loop(far * kinds, n * kinds - keep, drain_far, 0)
            pl.semaphore_signal(token, inc=1, device_id={"seq": z + 1})

    @pl.when(z < half // 2)
    def _():
        in_turn()

    @pl.when(z < n - 1)
    def _():
        final(z).wait_recv()

    my_count = blocks_ref[my_user]
    centers = [finals[0, pl.ds(k * users + my_user, 1), :] for k in range(kinds)]
    scales = [finals[1, pl.ds(k * users + my_user, 1), :] for k in range(kinds)]

    def normalise(s, carry):
        @pl.when(s == z)
        def _():
            own.wait()

        @pl.when(s != z)
        def _():
            for k in range(kinds):
                bulk(s, k, s).wait_recv()

        for k in range(kinds):
            for b in range(per_part):
                span = slice(b * BLOCK, (b + 1) * BLOCK)
                value = recv[k, s, span, :].astype(jnp.float32)
                scaled = (value - centers[k]) / scales[k]
                alive = s * per_dev + my_part * per_part + b < my_count
                out_ref[k, s, span, :] = jnp.where(alive, scaled, 0.0).astype(out_ref.dtype)
        return carry

    lax.fori_loop(0, z + 1, normalise, 0)

    @pl.when(jnp.logical_and(z >= half // 2, early))
    def _():
        in_turn()

    finals_ref[...] = finals[...]

    lax.fori_loop(z + 1, n, normalise, 0)

    @pl.when(z < n - 1)
    def _():
        prefix(z).wait_send()

    @pl.when(z == n - 1)
    def _():
        def drain_final(t, carry):
            final(t).wait_send()
            return carry

        lax.fori_loop(0, n - 1, drain_final, 0)

    def drain(t, carry):
        for k in range(kinds):
            waited = jnp.logical_and(
                jnp.logical_and(z < half - 1, t >= far), t * kinds + k < n * kinds - keep
            )

            @pl.when(jnp.logical_not(jnp.logical_or(waited, t == z)))
            def _(k=k):
                bulk(t, k).wait_send()
        return carry

    lax.fori_loop(0, n, drain, 0)


def on_device(kv_cache, valid_blocks):
    kinds, layer_dev, users, per_dev, heads_dev, head_dim = kv_cache.shape
    n = lax.axis_size("seq")
    part_len = per_dev // (n // users)
    kv = kv_cache.reshape(kinds, n, part_len, head_dim)
    whole = (kinds, n, part_len, head_dim)
    rows = kinds * users
    dma = pltpu.SemaphoreType.DMA
    out, finals = pl.pallas_call(
        functools.partial(exchange_kernel, n),
        out_shape=(
            jax.ShapeDtypeStruct(whole, kv.dtype),
            jax.ShapeDtypeStruct((2, rows, head_dim), jnp.float32),
        ),
        in_specs=[
            pl.BlockSpec(memory_space=pl.ANY),
            pl.BlockSpec(memory_space=pltpu.SMEM),
        ],
        out_specs=(
            pl.BlockSpec(memory_space=pltpu.VMEM),
            pl.BlockSpec(memory_space=pltpu.VMEM),
        ),
        scratch_shapes=[
            pltpu.VMEM(whole, kv.dtype),
            pltpu.VMEM(whole, kv.dtype),
            pltpu.VMEM((3, rows, head_dim), jnp.float32),
            pltpu.VMEM((3, rows, head_dim), jnp.float32),
            pltpu.VMEM((2, rows, head_dim), jnp.float32),
            dma,
            dma,
            dma((kinds, n)),
            dma((kinds, n)),
            dma,
            dma,
            dma((n,)),
            dma,
            pltpu.SemaphoreType.REGULAR((n,)),
            pltpu.SemaphoreType.REGULAR,
        ],
        compiler_params=pltpu.CompilerParams(collective_id=0, has_side_effects=True, vmem_limit_bytes=VMEM_LIMIT),
    )(kv, valid_blocks)
    arranged = out.reshape(kinds, layer_dev, 1, n * part_len, heads_dev, head_dim)
    small = (kinds, layer_dev, users, heads_dev, head_dim)
    return (arranged, finals[0].reshape(small), finals[1].reshape(small))


def solution(mesh):
    in_specs = (P(None, "layer", "groups", "seq", "head", None), P("groups"))
    out_specs = (
        P(None, "layer", ("groups", "seq"), None, "head", None),
        P(None, "layer", "groups", "head", None),
        P(None, "layer", "groups", "head", None),
    )
    return jax.shard_map(
        on_device, mesh=mesh, in_specs=in_specs, out_specs=out_specs, check_vma=False
    )
```

```python
import functools

import jax
import jax.numpy as jnp
from jax import lax
from jax.experimental import pallas as pl
from jax.experimental.pallas import tpu as pltpu
from jax.sharding import PartitionSpec as P

BLOCK = 128

epsilon = 1e-06
ceiling_value = 3e38
KEEP = (1, 2)
VMEM_LIMIT = 51 * 1024 * 1024


def exchange_kernel(
    n,
    kv_ref,
    blocks_ref,
    out_ref,
    finals_ref,
    local,
    recv,
    mine,
    gathered,
    finals,
    load_sem,
    own_sem,
    send_sem,
    recv_sem,
    stat_send_sem,
    stat_recv_sem,
    final_send_sem,
    final_recv_sem,
    ready,
    token,
):
    kinds, owners, part_len, head_dim = kv_ref.shape
    users = blocks_ref.shape[0]
    quarter = owners // users
    per_part = part_len // BLOCK
    per_dev = quarter * per_part
    rows = kinds * users
    half = n // 2
    z = lax.axis_index("seq")
    my_user, my_part = z // quarter, z % quarter
    early = z < half
    keep = jnp.where(z == 0, KEEP[0], KEEP[1])

    load = pltpu.make_async_copy(kv_ref, local, load_sem)
    load.start()
    own = pltpu.make_async_copy(kv_ref.at[:, z], recv.at[:, z], own_sem)
    own.start()

    barrier = pltpu.get_barrier_semaphore()

    @pl.when(z > 0)
    def _():
        pl.semaphore_wait(barrier, 1)

    @pl.when(z < n - 1)
    def _():
        pl.semaphore_signal(barrier, inc=1, device_id={"seq": z + 1})

    def announce(s, carry):
        pl.semaphore_signal(ready.at[z], inc=1, device_id={"seq": s})
        return carry

    lax.fori_loop(0, z, announce, 0)

    def bulk(t, k, s=None):
        s = z if s is None else s
        return pltpu.make_async_remote_copy(
            src_ref=kv_ref.at[k, t],
            dst_ref=recv.at[k, s],
            send_sem=send_sem.at[k, t],
            recv_sem=recv_sem.at[k, s],
            device_id={"seq": t},
        )

    def send_part(t, carry):
        for k in range(kinds):
            bulk(t, k).start()
        return carry

    late = jnp.logical_and(z >= half, z < n - 1)

    @pl.when(late)
    def _():
        send_part(0, 0)

    near = jnp.maximum(z - half + 1 - z % 2, 0)

    @pl.when(z < n - 1)
    def _():
        lax.fori_loop(near, z, send_part, 0)

    load.wait()

    def one_row(r, carry):
        k, u = r // users, r % users
        total = jnp.zeros((8, head_dim), jnp.float32)
        high = jnp.full((8, head_dim), -ceiling_value, jnp.float32)
        low = jnp.full((8, head_dim), ceiling_value, jnp.float32)
        count = blocks_ref[u]
        for b in range(per_dev):
            part = local[
                k,
                u * quarter + b // per_part,
                (b % per_part) * BLOCK : (b % per_part + 1) * BLOCK,
                :,
            ].astype(jnp.float32)
            part = part.reshape(BLOCK // 8, 8, head_dim)
            alive = z * per_dev + b < count
            total += jnp.where(alive, jnp.sum(part, axis=0), 0.0)
            high = jnp.maximum(high, jnp.where(alive, jnp.max(part, axis=0), -ceiling_value))
            low = jnp.minimum(low, jnp.where(alive, jnp.min(part, axis=0), ceiling_value))
        mine[0, pl.ds(r, 1), :] = jnp.sum(total, axis=0, keepdims=True)
        mine[1, pl.ds(r, 1), :] = jnp.max(high, axis=0, keepdims=True)
        mine[2, pl.ds(r, 1), :] = jnp.min(low, axis=0, keepdims=True)
        return carry

    lax.fori_loop(0, rows, one_row, 0)

    def prefix(s):
        return pltpu.make_async_remote_copy(
            src_ref=mine,
            dst_ref=gathered,
            send_sem=stat_send_sem,
            recv_sem=stat_recv_sem,
            device_id={"seq": s + 1},
        )

    @pl.when(z > 0)
    def _():
        prefix(z - 1).wait_recv()
        mine[0] = mine[0] + gathered[0]
        mine[1] = jnp.maximum(mine[1], gathered[1])
        mine[2] = jnp.minimum(mine[2], gathered[2])

    def final(t):
        return pltpu.make_async_remote_copy(
            src_ref=finals,
            dst_ref=finals,
            send_sem=final_send_sem.at[t],
            recv_sem=final_recv_sem,
            device_id={"seq": t},
        )

    @pl.when(z < n - 1)
    def _():
        pl.semaphore_wait(ready.at[z + 1], 1)
        prefix(z).start()

    @pl.when(z == n - 1)
    def _():
        row = lax.broadcasted_iota(jnp.int32, (rows, head_dim), 0)
        length = jnp.zeros((rows, head_dim), jnp.float32)
        for u in range(users):
            tokens = (blocks_ref[u] * BLOCK).astype(jnp.float32)
            length = jnp.where(row % users == u, tokens, length)
        center = mine[0] / length
        finals[0] = center
        finals[1] = jnp.maximum(mine[1] - center, center - mine[2]) + epsilon

        def send_final(t, carry):
            final(t).start()
            return carry

        lax.fori_loop(0, n - 1, send_final, 0)

    lax.fori_loop(jnp.where(late, 1, 0), near, send_part, 0)

    @pl.when(z == n - 1)
    def _():
        lax.fori_loop(near, z, send_part, 0)

    far = z + half + 1 - z % 2

    def send_upper(t, carry):
        @pl.when(t > z + 1)
        def _():
            pl.semaphore_wait(ready.at[t], 1)

        @pl.when(jnp.logical_and(early, jnp.logical_or(t <= half, jnp.logical_and(z == 0, t >= far))))
        def _():
            send_part(t, 0)

        release = n - quarter
        begin = jnp.where(t > release, t, jnp.maximum(z, half) + 1)

        @pl.when(t >= release)
        def _():
            lax.fori_loop(begin, jnp.minimum(far, t + 1), send_part, 0)

        return carry

    lax.fori_loop(z + 1, n, send_upper, 0)

    def in_turn():
        @pl.when(z > 0)
        def _():
            pl.semaphore_wait(token, 1)
            lax.fori_loop(far, n, send_part, 0)

        @pl.when(z < half - 1)
        def _():
            def drain_far(i, carry):
                bulk(i // kinds, i % kinds).wait_send()
                return carry

            lax.fori_loop(far * kinds, n * kinds - keep, drain_far, 0)
            pl.semaphore_signal(token, inc=1, device_id={"seq": z + 1})

    @pl.when(z < half // 2)
    def _():
        in_turn()

    @pl.when(z < n - 1)
    def _():
        final(z).wait_recv()

    my_count = blocks_ref[my_user]
    centers = [finals[0, pl.ds(k * users + my_user, 1), :] for k in range(kinds)]
    scales = [finals[1, pl.ds(k * users + my_user, 1), :] for k in range(kinds)]

    def normalise(s, carry):
        @pl.when(s == z)
        def _():
            own.wait()

        @pl.when(s != z)
        def _():
            for k in range(kinds):
                bulk(s, k, s).wait_recv()

        for k in range(kinds):
            for b in range(per_part):
                span = slice(b * BLOCK, (b + 1) * BLOCK)
                value = recv[k, s, span, :].astype(jnp.float32)
                scaled = (value - centers[k]) / scales[k]
                alive = s * per_dev + my_part * per_part + b < my_count
                out_ref[k, s, span, :] = jnp.where(alive, scaled, 0.0).astype(out_ref.dtype)
        return carry

    lax.fori_loop(0, z + 1, normalise, 0)

    @pl.when(jnp.logical_and(z >= half // 2, early))
    def _():
        in_turn()

    finals_ref[...] = finals[...]

    lax.fori_loop(z + 1, n, normalise, 0)

    @pl.when(z < n - 1)
    def _():
        prefix(z).wait_send()

    @pl.when(z == n - 1)
    def _():
        def drain_final(t, carry):
            final(t).wait_send()
            return carry

        lax.fori_loop(0, n - 1, drain_final, 0)

    def drain(t, carry):
        for k in range(kinds):
            waited = jnp.logical_and(
                jnp.logical_and(z < half - 1, t >= far), t * kinds + k < n * kinds - keep
            )

            @pl.when(jnp.logical_not(jnp.logical_or(waited, t == z)))
            def _(k=k):
                bulk(t, k).wait_send()
        return carry

    lax.fori_loop(0, n, drain, 0)


def on_device(kv_cache, valid_blocks):
    kinds, layer_dev, users, per_dev, heads_dev, head_dim = kv_cache.shape
    n = lax.axis_size("seq")
    part_len = per_dev // (n // users)
    kv = kv_cache.reshape(kinds, n, part_len, head_dim)
    whole = (kinds, n, part_len, head_dim)
    rows = kinds * users
    dma = pltpu.SemaphoreType.DMA
    out, finals = pl.pallas_call(
        functools.partial(exchange_kernel, n),
        out_shape=(
            jax.ShapeDtypeStruct(whole, kv.dtype),
            jax.ShapeDtypeStruct((2, rows, head_dim), jnp.float32),
        ),
        in_specs=[
            pl.BlockSpec(memory_space=pl.ANY),
            pl.BlockSpec(memory_space=pltpu.SMEM),
        ],
        out_specs=(
            pl.BlockSpec(memory_space=pltpu.VMEM),
            pl.BlockSpec(memory_space=pltpu.VMEM),
        ),
        scratch_shapes=[
            pltpu.VMEM(whole, kv.dtype),
            pltpu.VMEM(whole, kv.dtype),
            pltpu.VMEM((3, rows, head_dim), jnp.float32),
            pltpu.VMEM((3, rows, head_dim), jnp.float32),
            pltpu.VMEM((2, rows, head_dim), jnp.float32),
            dma,
            dma,
            dma((kinds, n)),
            dma((kinds, n)),
            dma,
            dma,
            dma((n,)),
            dma,
            pltpu.SemaphoreType.REGULAR((n,)),
            pltpu.SemaphoreType.REGULAR,
        ],
        compiler_params=pltpu.CompilerParams(collective_id=0, has_side_effects=True, vmem_limit_bytes=VMEM_LIMIT),
    )(kv, valid_blocks)
    arranged = out.reshape(kinds, layer_dev, 1, n * part_len, heads_dev, head_dim)
    small = (kinds, layer_dev, users, heads_dev, head_dim)
    return (arranged, finals[0].reshape(small), finals[1].reshape(small))


def solution(mesh):
    in_specs = (P(None, "layer", "groups", "seq", "head", None), P("groups"))
    out_specs = (
        P(None, "layer", ("groups", "seq"), None, "head", None),
        P(None, "layer", "groups", "head", None),
        P(None, "layer", "groups", "head", None),
    )
    return jax.shard_map(
        on_device, mesh=mesh, in_specs=in_specs, out_specs=out_specs, check_vma=False
    )
```
